32 devices in a mesh: pert: 2 (over x), ga: 16 (over z, y, core).
Axes of the slice: x: 2, y: 2, z: 4, core: 2. Of those that a mesh axis runs over, the one named last changes fastest.
Arguments:
- psi_k: bfloat16 [2, 8192, 256], P(None, 'ga'), may hold values from -6 to 6
- beta_k: bfloat16 [2, 8192, 2496], P(None, 'ga'), may hold values from -0.0625 to 0.0625
- beta_kq: bfloat16 [2, 8192, 2496], P(None, 'ga'), may hold values from -0.15625 to 0.15625
- g_k: float32 [3, 8192], P(None, 'ga'), may hold values from -2 to 2
- g_kq: float32 [3, 8192], P(None, 'ga'), may hold values from -2 to 2
- send_index: int32 [16, 16, 32], P('ga'), may hold values from -1 to 511, as said below
- recv_index: int32 [8192], P('ga'), may hold values from -1 to 511, as said below
- dmat: float32 [192, 13, 13], replicated, may hold values from -0.5 to 4, as said below
- displaced: int32 [256], P('pert'), parts along dimension 0, may hold values from 0 to 191, as said below
- mode: float32 [3, 256], P(None, 'pert'), parts along dimension 1, may hold values from -5 to 5
Outputs:
- dvpsi: bfloat16 [4, 8192, 256], P('pert', 'ga'), parts along dimension 0
The draws below stay inside these ranges and needn't reach their ends.
There are 2 independent parts, one for each index of `pert`. The reference program is written for one: setup_inputs(seed, part) draws one part's arguments, and reference() takes and returns one part's arrays. A program takes and returns all parts, laid end to end along the dimension named above; an argument that names none is the same for every part. Nothing has to cross between parts.
Inputs may be any that keep to these rules, and one draw needn't show every extreme that they name: `send_index`: entry [s, d, c] is a row of device s's k-sphere block in local numbering, or -1 for an unused slot; the rows device s sends are distinct; in every draw some device receives 32 rows from every device. `recv_index`: entry r is s * 32 + c, naming slot c from device s among the rows received by the device of row r, or -1 for a row with no k-sphere counterpart; every used slot is named by exactly one row of its receiving device and no unused slot is named. `dmat`: each atom's block is symmetric. `displaced`: 128 distinct atoms.
All inputs are finite; a program needn't handle non-finite values.
Results may differ from the reference program's by a relative error of at most 0.0057.
Values may be sent and summed in bfloat16 or wider, within the bound.
A program may use at most 128 MiB of HBM per device.

```python
import jax
import jax.numpy as jnp
from jax import lax

KQ_DEV = 512
NB = 256
NPROJ_ATOM = 13
ATOMS = 192
DISP = 128
CAP = 32
NPW_Q = 8192
NPROJ = 2496
N_GA = 16


def exchange_plan(key):
    base = jax.random.fold_in(key, 7)
    key_counts, key_full, key_send, key_rows = jax.random.split(base, 4)
    short_draw = jax.random.randint(key_counts, (N_GA, N_GA), 0, 10)
    counts = jnp.where(short_draw == 0, CAP - 1, CAP)
    full_target = jax.random.randint(key_full, (), 0, N_GA)
    counts = jnp.where(jnp.arange(N_GA)[None, :] == full_target, CAP, counts).astype(jnp.int32)
    send_order = jax.vmap(lambda single: jax.random.permutation(single, KQ_DEV))(jax.random.split(key_send, N_GA)).astype(jnp.int32)
    slot_ids = jnp.arange(CAP, dtype=jnp.int32)
    offsets = jnp.cumsum(counts, axis=1) - counts
    positions = jnp.minimum(offsets[:, :, None] + slot_ids[None, None, :], KQ_DEV - 1).reshape(N_GA, N_GA * CAP)
    sent_rows = jnp.take_along_axis(send_order, positions, axis=1).reshape(N_GA, N_GA, CAP)
    live_slots = slot_ids[None, None, :] < counts[:, :, None]
    send_table = jnp.where(live_slots, sent_rows, -1).astype(jnp.int32)
    live_dest = jnp.transpose(live_slots, (1, 0, 2)).reshape(N_GA, N_GA * CAP)
    live_order = jnp.argsort(jnp.where(live_dest, 0, 1).astype(jnp.int32), axis=1, stable=True).astype(jnp.int32)
    live_total = jnp.sum(live_dest.astype(jnp.int32), axis=1)
    padded_order = jnp.concatenate([live_order, jnp.zeros((N_GA, KQ_DEV - N_GA * CAP), jnp.int32)], axis=1)
    row_ids = jnp.arange(KQ_DEV, dtype=jnp.int32)
    buffer_vals = jnp.where(row_ids[None, :] < live_total[:, None], padded_order, -1).astype(jnp.int32)
    row_perms = jax.vmap(lambda single: jax.random.permutation(single, KQ_DEV))(jax.random.split(key_rows, N_GA)).astype(jnp.int32)
    recv_table = jnp.zeros((N_GA, KQ_DEV), jnp.int32).at[jnp.arange(N_GA)[:, None], row_perms].set(buffer_vals)
    return (send_table, recv_table.reshape(-1))


def draw_send_index(key, part):
    send_table, recv_table = exchange_plan(key)
    return send_table


def draw_recv_index(key, part):
    send_table, recv_table = exchange_plan(key)
    return recv_table


def draw_dmat(key, part):
    key_off, key_diag = jax.random.split(jax.random.fold_in(key, 11))
    raw = jnp.clip(0.3 * jax.random.normal(key_off, (ATOMS, NPROJ_ATOM, NPROJ_ATOM), jnp.float32), -0.5, 0.5)
    symmetric = 0.5 * (raw + jnp.swapaxes(raw, 1, 2))
    diagonal = jax.random.uniform(key_diag, (ATOMS, NPROJ_ATOM), jnp.float32, 0.5, 2.5)
    identity = jnp.eye(NPROJ_ATOM, dtype=jnp.float32)
    return symmetric * (1.0 - identity) + diagonal[:, :, None] * identity


def draw_displaced(key, part):
    chosen = jax.random.permutation(jax.random.fold_in(key, 13), ATOMS)
    return chosen[:DISP].astype(jnp.int32)


def shard_levels(stream_key, shape, cuts, smallest, high):
    loudness = 1.0
    for dim, parts in cuts:
        steps = jax.random.uniform(jax.random.fold_in(jax.random.fold_in(stream_key, 6), dim), (parts,), jnp.float32, smallest / len(cuts), high / len(cuts))
        loudness = loudness * jnp.repeat(jnp.exp(steps), shape[dim] // parts).reshape((-1,) + (1,) * (len(shape) - 1 - dim))
    return loudness


def bell_draw(key, shape, deviation, most, cuts=(), kind=jnp.bfloat16):
    result = jax.random.normal(key, shape, jnp.float32) * deviation
    if len(cuts) > 0:
        result = shard_levels(key, shape, cuts, -0.22, 0.18) * result
    return jnp.clip(result, min=-most, max=most).astype(kind)


def setup_inputs(seed: int = 0, part: int = 0) -> dict:
    arg_keys = jax.random.split(jax.random.key(seed), 11)
    own_keys = jax.random.split(jax.random.fold_in(arg_keys[10], part), 11)
    psi_k = bell_draw(arg_keys[0], (2, NPW_Q, NB), 1.0, 6.0, ((1, 16),))
    beta_k = bell_draw(arg_keys[1], (2, NPW_Q, NPROJ), NPW_Q ** -0.5, 0.0625, ((1, 16),))
    beta_kq = bell_draw(arg_keys[2], (2, NPW_Q, NPROJ), (DISP * NPROJ_ATOM) ** -0.5, 0.15625, ((1, 16),))
    g_k = jnp.clip(jax.random.uniform(arg_keys[3], (3, NPW_Q), jnp.float32, -2.0, 2.0) * shard_levels(arg_keys[3], (3, NPW_Q), ((1, 16),), -0.4, 0.0), -2.0, 2.0)
    g_kq = jnp.clip(jax.random.uniform(arg_keys[4], (3, NPW_Q), jnp.float32, -2.0, 2.0) * shard_levels(arg_keys[4], (3, NPW_Q), ((1, 16),), -0.4, 0.0), -2.0, 2.0)
    send_index = draw_send_index(jax.random.fold_in(arg_keys[10], 71), part)
    recv_index = draw_recv_index(jax.random.fold_in(arg_keys[10], 71), part)
    dmat = draw_dmat(jax.random.fold_in(arg_keys[10], 71), part)
    displaced = draw_displaced(jax.random.fold_in(jax.random.fold_in(arg_keys[10], part), 71), part)
    mode = bell_draw(own_keys[9], (3, DISP), 1.0, 5.0, (), jnp.float32)
    return dict(psi_k=psi_k, beta_k=beta_k, beta_kq=beta_kq, g_k=g_k, g_kq=g_kq, send_index=send_index, recv_index=recv_index, dmat=dmat, displaced=displaced, mode=mode)


def contract_rows(left_side, stacked):
    return lax.dot_general(left_side, stacked, (((0,), (0,)), ((), ())), preferred_element_type=jnp.float32)


def local_terms(wave_rows, beta_rows, g_vectors, columns, weights):
    band_count = wave_rows.shape[2]
    picked = jnp.take(beta_rows, columns, axis=2)
    row_scale = jnp.dot(g_vectors.T, weights, precision=lax.Precision.HIGHEST, preferred_element_type=jnp.float32)
    conj_real = (row_scale * picked[1]).astype(jnp.bfloat16)
    conj_imag = (row_scale * picked[0]).astype(jnp.bfloat16)
    stacked = jnp.concatenate([wave_rows[0], wave_rows[1]], axis=1)
    with_real = contract_rows(picked[0], stacked)
    with_imag = contract_rows(picked[1], stacked)
    slope_real = contract_rows(conj_real, stacked)
    slope_imag = contract_rows(conj_imag, stacked)
    plain_part = jnp.stack([with_real[:, :band_count] + with_imag[:, band_count:],
                            with_real[:, band_count:] - with_imag[:, :band_count]])
    slope_part = jnp.stack([slope_real[:, :band_count] - slope_imag[:, band_count:],
                            slope_real[:, band_count:] + slope_imag[:, :band_count]])
    return jnp.stack([plain_part, slope_part])


def couple_atoms(summed, coupling):
    shape_in = summed.shape
    blocks = summed.reshape(2, 2, coupling.shape[0], coupling.shape[1], shape_in[3])
    mixed = jnp.einsum("dij,xcdjn->xcdin", coupling, blocks, precision=lax.Precision.HIGHEST)
    return mixed.reshape(shape_in).astype(jnp.bfloat16)


def back_project(coupled, beta_rows, g_vectors, columns, weights):
    band_count = coupled.shape[3]
    picked = jnp.take(beta_rows, columns, axis=2)
    row_scale = jnp.dot(g_vectors.T, weights, precision=lax.Precision.HIGHEST, preferred_element_type=jnp.float32)
    slope_real = (row_scale * picked[1]).astype(jnp.bfloat16)
    slope_imag = (-row_scale * picked[0]).astype(jnp.bfloat16)
    left_side = jnp.concatenate([slope_real, slope_imag, picked[0], picked[1]], axis=1)
    bra_terms = coupled[0]
    ket_terms = coupled[1]
    real_part = jnp.concatenate([bra_terms[0], -bra_terms[1], ket_terms[0], -ket_terms[1]], axis=0)
    imag_part = jnp.concatenate([bra_terms[1], bra_terms[0], ket_terms[1], ket_terms[0]], axis=0)
    right_side = jnp.concatenate([real_part, imag_part], axis=1)
    product = jnp.dot(left_side, right_side, preferred_element_type=jnp.float32)
    return jnp.stack([product[:, :band_count], product[:, band_count:]]).astype(jnp.bfloat16)


def reference(psi_k, beta_k, beta_kq, g_k, g_kq, send_index, recv_index, dmat, displaced, mode):
    row_total = recv_index.shape[0]
    row_ids = jnp.arange(row_total, dtype=jnp.int32)
    target = (row_ids // KQ_DEV).astype(jnp.int32)
    buffer_pos = jnp.maximum(recv_index, 0).astype(jnp.int32)
    source = (buffer_pos // CAP).astype(jnp.int32)
    slot_ids = (buffer_pos % CAP).astype(jnp.int32)
    local_row = send_index[source, target, slot_ids]
    live_rows = (recv_index >= 0) & (local_row >= 0)
    anchor = (source * KQ_DEV + jnp.maximum(local_row, 0)).astype(jnp.int32)
    psi_kq = jnp.where(live_rows[None, :, None], psi_k[:, anchor, :], jnp.zeros((), psi_k.dtype))
    columns = (displaced[:, None] * NPROJ_ATOM + jnp.arange(NPROJ_ATOM, dtype=jnp.int32)[None, :]).reshape(-1).astype(jnp.int32)
    atom_of = jnp.repeat(jnp.arange(DISP, dtype=jnp.int32), NPROJ_ATOM)
    weights = mode[:, atom_of]
    proj_count = columns.shape[0]

    def project_block(running, block_id):
        row_start = (block_id * KQ_DEV).astype(jnp.int32)
        wave_rows = lax.dynamic_slice_in_dim(psi_kq, row_start, KQ_DEV, 1)
        beta_rows = lax.dynamic_slice_in_dim(beta_k, row_start, KQ_DEV, 1)
        g_vectors = lax.dynamic_slice_in_dim(g_k, row_start, KQ_DEV, 1)
        return running + local_terms(wave_rows, beta_rows, g_vectors, columns, weights), None

    start_sum = jnp.zeros((2, 2, proj_count, NB), jnp.float32)
    summed, unused = lax.scan(project_block, start_sum, jnp.arange(N_GA, dtype=jnp.int32))
    coupling = jnp.take(dmat, displaced, axis=0)
    coupled = couple_atoms(summed, coupling)

    def apply_block(block_id):
        row_start = (block_id * KQ_DEV).astype(jnp.int32)
        beta_rows = lax.dynamic_slice_in_dim(beta_kq, row_start, KQ_DEV, 1)
        g_vectors = lax.dynamic_slice_in_dim(g_kq, row_start, KQ_DEV, 1)
        return back_project(coupled, beta_rows, g_vectors, columns, weights)

    pieces = lax.map(apply_block, jnp.arange(N_GA, dtype=jnp.int32))
    return jnp.transpose(pieces, (1, 0, 2, 3)).reshape(2, row_total, NB)
```

```python
import functools

import jax
import jax.numpy as jnp
import numpy as np
from jax import lax
from jax.experimental import pallas as pl
from jax.experimental.pallas import tpu as pltpu
from jax.sharding import PartitionSpec as P

LANES = 128
RING = 4
CORE_Y = 4
LINE = 4
BLOCKS = 4
COPIES = 120
EARLY = 2
FILL = (5.6, 5.7, 7.8, 10.0)
BF16 = jnp.bfloat16
F32 = jnp.float32
VMEM_LIMIT = 56 * 1024 * 1024


def round_up(value, step):
    return -(-value // step) * step


def dot(a, b):
    return jnp.dot(a, b, preferred_element_type=F32)


def dot_t(a, b):
    return lax.dot_general(a, b, (((0,), (0,)), ((), ())), preferred_element_type=F32)


def pack_kernel(slot_ref, psi_ref, out_ref):
    rows = psi_ref.shape[1]
    bands = psi_ref.shape[2]
    slots = slot_ref.shape[1]
    pick = (lax.broadcasted_iota(jnp.int32, (rows, slots), 0) == slot_ref[...]).astype(BF16)
    for part in range(2):
        out_ref[:, part * bands:(part + 1) * bands] = dot_t(pick, psi_ref[part]).astype(BF16)


def pack_rows(slots, psi_k):
    return pl.pallas_call(
        pack_kernel,
        out_shape=jax.ShapeDtypeStruct((slots.shape[1], 2 * psi_k.shape[2]), BF16),
        compiler_params=pltpu.CompilerParams(vmem_limit_bytes=VMEM_LIMIT),
    )(slots, psi_k)


class Layout:
    def __init__(self, groups, atoms, per_atom, total):
        self.groups = groups
        self.blocks = groups // CORE_Y
        self.gang = CORE_Y
        if self.blocks != RING:
            self.blocks = RING
            self.gang = groups // RING
        self.per_shard = atoms // groups
        self.per_atom = per_atom
        self.used = self.per_shard * per_atom
        self.rows = round_up(self.used, 16)
        self.block = self.gang * self.rows
        self.padded = round_up(self.block, LANES)
        self.total = total
        slack = total - atoms * per_atom
        self.window = min(total, round_up(self.gang * self.used + slack + 16, LANES))
        self.starts = [
            min(b * self.gang * self.used // 16 * 16, total - self.window) for b in range(self.blocks)
        ]


def columns_of(layout, info_ref, b):
    wide = info_ref[:, b * layout.padded:(b + 1) * layout.padded]
    return jnp.transpose(wide)[: layout.block]


def select(layout, beta_ref, info, b):
    start = layout.starts[b]
    ids = lax.broadcasted_iota(jnp.int32, (info.shape[0], layout.window), 1) + start
    pick = (ids == info[:, 0:1].astype(jnp.int32)).astype(BF16)
    rows = pl.ds(start, layout.window)
    return dot(pick, beta_ref[0, rows, :]), dot(pick, beta_ref[1, rows, :])


def row_scale(g_ref, info):
    total = info[:, 1:2] * g_ref[0:1, :]
    for x in range(1, g_ref.shape[0]):
        total = total + info[:, x + 1:x + 2] * g_ref[x:x + 1, :]
    return total


def regroup(arrived_ref, slot_ref, wave):
    slots, rows = arrived_ref.shape[0], wave.shape[0]
    pick = (lax.broadcasted_iota(jnp.int32, (slots, rows), 0) == slot_ref[...]).astype(BF16)
    wave[...] = dot_t(pick, arrived_ref[...]).astype(BF16)


def selected_terms(layout, beta_ref, info, g_ref, b):
    real, imag = select(layout, beta_ref, info, b)
    scale = row_scale(g_ref, info)
    return real, imag, scale * imag, scale * real


def project_block(terms, stacked, store):
    bands = stacked.shape[1] // 2
    x = dot(terms[0], stacked)
    y = dot(terms[1], stacked)
    store(0, (x[:, :bands] + y[:, bands:]).astype(BF16))
    store(1, (x[:, bands:] - y[:, :bands]).astype(BF16))
    x = dot(terms[2], stacked)
    y = dot(terms[3], stacked)
    store(2, (x[:, :bands] - y[:, bands:]).astype(BF16))
    store(3, (x[:, bands:] + y[:, :bands]).astype(BF16))


def prepare_block(layout, beta_ref, info, g_ref, left_ref, b):
    real, imag, slope_real, slope_imag = selected_terms(layout, beta_ref, info, g_ref, b)
    for k, term in enumerate((slope_real, -slope_imag, real, imag)):
        left_ref[b, k] = term.astype(BF16).T


def back_block(left_ref, b, coupled):
    width = coupled.shape[1] // 2
    bands = width // 2
    first, second = coupled[:, :width], coupled[:, width:]
    x = dot(left_ref[b, 0], first) + dot(left_ref[b, 2], second)
    y = dot(left_ref[b, 1], first) + dot(left_ref[b, 3], second)
    return x[:, :bands] - y[:, bands:], x[:, bands:] + y[:, :bands]


def project_kernel(layout, arrived_ref, slot_ref, beta_ref, info_ref, g_ref, out_ref, wave):
    regroup(arrived_ref, slot_ref, wave)
    bands = wave.shape[1] // 2
    for b in range(layout.blocks):

        def store(k, value, b=b):
            out_ref[b * layout.block:(b + 1) * layout.block, k * bands:(k + 1) * bands] = value

        info = columns_of(layout, info_ref, b)
        terms = [term.astype(BF16) for term in selected_terms(layout, beta_ref, info, g_ref, b)]
        project_block(terms, wave[...], store)


def finish_kernel(layout, beta_ref, info_ref, g_ref, coupled_ref, out_ref, left, total):
    for b in range(layout.blocks):
        prepare_block(layout, beta_ref, columns_of(layout, info_ref, b), g_ref, left, b)
        parts = back_block(left, b, coupled_ref[b * layout.block:(b + 1) * layout.block, :])
        for k in range(2):
            total[k] = parts[k] if b == 0 else total[k] + parts[k]
    out_ref[...] = total[...].astype(BF16)


def params(**extra):
    return pltpu.CompilerParams(vmem_limit_bytes=VMEM_LIMIT, **extra)


def separate_steps(layout, arrived, slots, beta_k, beta_kq, info, g_k, g_kq, coupling):
    rows, width = slots.shape[1], arrived.shape[1]
    terms = pl.pallas_call(
        functools.partial(project_kernel, layout),
        out_shape=jax.ShapeDtypeStruct((layout.groups * layout.rows, 2 * width), BF16),
        scratch_shapes=[pltpu.VMEM((rows, width), BF16)],
        compiler_params=params(),
    )(arrived, slots, beta_k, info, g_k)
    shard = lax.psum_scatter(terms.astype(F32), "ga", scatter_dimension=0, tiled=True)
    mixed = jnp.dot(
        coupling, shard, precision=lax.Precision.HIGHEST, preferred_element_type=F32
    ).astype(BF16)
    coupled = lax.all_gather(mixed, "ga", axis=0, tiled=True)
    return pl.pallas_call(
        functools.partial(finish_kernel, layout),
        out_shape=jax.ShapeDtypeStruct((2, rows, width // 2), BF16),
        scratch_shapes=[
            pltpu.VMEM((layout.blocks, 4, rows, layout.block), BF16),
            pltpu.VMEM((2, rows, width // 2), F32),
        ],
        compiler_params=params(),
    )(beta_kq, info, g_kq, coupled)


class Plan:
    def __init__(self, atoms, per_atom, total):
        self.per_atom = per_atom
        self.atoms = atoms // BLOCKS
        self.rows = self.atoms * per_atom
        self.half = self.rows // 2
        slack = total - atoms * per_atom
        self.window = min(total, round_up(self.rows + slack + 16, LANES))
        self.starts = [min(b * self.rows // 16 * 16, total - self.window) for b in range(BLOCKS)]


class Flow:
    def __init__(self, wire, target, device):
        self.k = wire.count
        wire.count += 1
        self.wire, self.target, self.device = wire, target, device

    def copy(self, source):
        return pltpu.make_async_remote_copy(
            src_ref=source,
            dst_ref=self.target,
            send_sem=self.wire.send_sem.at[self.k],
            recv_sem=self.wire.recv_sem.at[self.k],
            device_id={"ga": self.device},
            device_id_type=pl.DeviceIdType.MESH,
        )

    def start(self, source):
        self.copy(source).start()

    def arrived(self):
        self.copy(self.target).wait_recv()

    def sent(self):
        self.copy(self.target).wait_send()


class Wire:
    def __init__(self, send_sem, recv_sem):
        self.send_sem, self.recv_sem, self.count = send_sem, recv_sem, 0


def exact_dot(a, b):
    return jnp.dot(a, b, precision=lax.Precision.HIGHEST, preferred_element_type=F32)


def slot_row(send_ref):
    receivers, cap = send_ref.shape
    column = lax.broadcasted_iota(jnp.int32, (cap, receivers * cap), 1)
    inner = lax.broadcasted_iota(jnp.int32, (cap, receivers * cap), 0)
    wide = exact_dot(send_ref[...].astype(F32), (column % cap == inner).astype(F32))
    column = lax.broadcasted_iota(jnp.int32, wide.shape, 1)
    outer = lax.broadcasted_iota(jnp.int32, wide.shape, 0)
    return jnp.sum(jnp.where(column // cap == outer, wide, 0.0), axis=0, keepdims=True).astype(jnp.int32)


def split_exact(value):
    parts = []
    for _ in range(3):
        parts.append(value.astype(BF16))
        value = value - parts[-1].astype(F32)
    return parts


def divide(index, by):
    return jnp.floor((index.astype(F32) + 0.5) * (1.0 / by))


def sorted_info(plan, displaced_ref, mode_ref, values, info):
    parts = mode_ref.shape[0]
    values[...] = jnp.zeros_like(values)
    values[0:1, :] = displaced_ref[...].astype(F32)
    values[1:1 + parts, :] = mode_ref[...]
    by_atom = jnp.transpose(values[...])
    smaller = (by_atom[:, 0:1] < values[0:1, :]).astype(F32)
    rank = jnp.sum(smaller, axis=0, keepdims=True)
    pieces = split_exact(by_atom)
    row = lax.broadcasted_iota(jnp.int32, (plan.rows, 1), 0)
    slot = divide(row, plan.per_atom)
    proj = row.astype(F32) - slot * plan.per_atom
    lane = lax.broadcasted_iota(jnp.int32, (plan.rows, values.shape[0]), 1)
    for b in range(BLOCKS):
        pick = (slot + float(b * plan.atoms) == rank).astype(BF16)
        found = dot(pick, pieces[0]) + dot(pick, pieces[1]) + dot(pick, pieces[2])
        source = found * plan.per_atom + proj
        info[b] = jnp.where(lane == 0, source, jnp.where(lane == 7, found[:, 0:1], found))


def coupling_matrix(plan, dmat_ref, spread, atom):
    count, step = plan.per_atom, round_up(plan.per_atom, 8)
    spread[...] = jnp.zeros_like(spread)
    for i in range(count):
        spread[i * step:i * step + count, :] = dmat_ref[i]
    row = lax.broadcasted_iota(jnp.int32, (plan.half, 1), 0)
    slot = divide(row, count)
    proj = row.astype(F32) - slot * count
    column = lax.broadcasted_iota(jnp.int32, (1, plan.half), 1)
    column_slot = divide(column, count)
    column_proj = column.astype(F32) - column_slot * count
    lanes = lax.broadcasted_iota(jnp.int32, (plan.half, spread.shape[1]), 1).astype(F32)
    found = lax.dot_general(
        (lanes == atom).astype(F32), spread[...], (((1,), (1,)), ((), ())),
        precision=lax.Precision.HIGHEST, preferred_element_type=F32,
    )
    wide = lax.broadcasted_iota(jnp.int32, (1, count * step), 1)
    found = jnp.where((wide // step).astype(F32) == proj, found, 0.0)
    tall = lax.broadcasted_iota(jnp.int32, (count * step, 1), 0)
    move = ((tall % step).astype(F32) == column_proj).astype(F32)
    return jnp.where(slot == column_slot, exact_dot(found, move), 0.0)


def far_first(n):
    return sorted(range(1, n), key=lambda step: -min(step, n - step))


KINDS = ("A", "B")
UNITS = [("B", q, yy, part) for q in range(1) for yy in range(2) for part in range(2)]
UNITS += [("A", 0, 0, part) for part in range(2)]
UNITS += [("B", 1, yy, part) for yy in range(2) for part in range(2)]
UNITS += [("A", 1, 0, part) for part in range(2)]
SHARES = [(kind, q, part) for q in range(2) for kind in ("A", "O", "P") for part in range(2)]
UNIT = 1.14
HOP = 3.1
COMPUTE = 1.35


def fused_kernel(
    plan, psi_ref, send_ref, slot_ref, displaced_ref, mode_ref, g_k_ref, g_kq_ref, dmat_ref, beta_k_hbm, beta_kq_hbm,
    out_ref, wave, terms, left, mine, y_in, y_sum, side_in, mid_in, yb_in, shared, total, stage, out_in,
    beta_k, beta_kq, packed, arrived, slot_in, g_in, values, info, spread, coupling, send_sem, recv_sem, load_sem,
):
    me = lax.axis_index("ga")
    n = 2 * 2 * LINE
    c, y, z = me % 2, (me // 2) % 2, me // 4
    chip = me // 2
    outer, inner = z % 3 == 0, z % 3 != 0
    is_outer = (2 - z % 3) // 2
    near, far = z // 2, 1 - z // 2

    def index(zz, yy, cc):
        return (zz * 2 + yy) * 2 + cc

    other_core, other_y = index(z, y, 1 - c), index(z, 1 - y, c)
    side, mid = index(z + 1 - 2 * (z % 2), y, c), index(LINE - 1 - z, y, c)
    load_k = pltpu.make_async_copy(beta_k_hbm, beta_k, load_sem.at[0])
    load_k.start()
    load = pltpu.make_async_copy(beta_kq_hbm, beta_kq, load_sem.at[1])
    load.start()

    barrier = pltpu.get_barrier_semaphore()
    for step in range(1, n):
        pl.semaphore_signal(
            barrier, inc=1, device_id={"ga": (me + step) % n}, device_id_type=pl.DeviceIdType.MESH
        )
    rows = psi_ref.shape[1]
    cap = send_ref.shape[1]
    slots = n * cap
    hb = psi_ref.shape[2] // 2
    width = 2 * hb
    half = plan.half
    pick = (lax.broadcasted_iota(jnp.int32, (rows, slots), 0) == slot_row(send_ref)).astype(BF16)
    for part in range(2):
        moved = dot_t(pick, psi_ref[part]).astype(BF16).reshape(n // 2, 2, cap, 2 * hb)
        for cc in range(2):
            packed[:, cc, :, :, part * hb:(part + 1) * hb] = moved[:, :, :, cc * hb:(cc + 1) * hb]
    pl.semaphore_wait(barrier, n - 1)

    wire = Wire(send_sem, recv_sem)

    def flow(target, device):
        return Flow(wire, target, device)

    flows = []
    psi_flows = []
    for step in far_first(n):
        to = (me + step) % n
        psi_flows.append(flow(arrived.at[:, me], to))
        psi_flows[-1].start(packed.at[to // 2, to % 2])
    slot_flow, g_flow = flow(slot_in, other_core), flow(g_in, other_core)
    slot_flow.start(slot_ref)
    g_flow.start(g_k_ref)
    for j in range(2):
        arrived[j, me] = packed[chip, c, j]

    sorted_info(plan, displaced_ref, mode_ref, values, info)
    load_k.wait()
    own_rows, peer_rows = pl.ds(0, rows), pl.ds(rows, rows)
    term_flows = []

    def slopes(b, g_ref, at):
        scale = row_scale(g_ref, info[b])
        terms[b, 2, :, at] = (scale * terms[b, 1, :, at].astype(F32)).astype(BF16)
        terms[b, 3, :, at] = (scale * terms[b, 0, :, at].astype(F32)).astype(BF16)

    for b in range(BLOCKS):
        for k, value in enumerate(select(plan, beta_k, info[b], b)):
            terms[b, k, :, own_rows] = value.astype(BF16)
        term_flows.append(flow(terms.at[b, pl.ds(0, 2), :, peer_rows], other_core))
        term_flows[b].start(terms.at[b, pl.ds(0, 2), :, own_rows])
        slopes(b, g_k_ref, own_rows)
        if b == 0:
            g_flow.arrived()
        else:
            term_flows[b - 1].arrived()
            slopes(b - 1, g_in, peer_rows)
    term_flows[BLOCKS - 1].arrived()
    slopes(BLOCKS - 1, g_in, peer_rows)

    left_flows = []

    def prepare(b):
        if b == 0:
            load.wait()
        real, imag = select(plan, beta_kq, info[b], b)
        scale = row_scale(g_kq_ref, info[b])
        for k, term in enumerate((scale * imag, -(scale * real), real, imag)):
            left[b, k, own_rows] = term.astype(BF16).T
        left_flows.append(flow(left.at[b, :, peer_rows], other_core))
        left_flows[b].start(left.at[b, :, own_rows])

    for b in range(EARLY):
        prepare(b)

    slot_flow.arrived()
    for copy in psi_flows:
        copy.arrived()
    for h, ref, owner in ((0, slot_ref, c), (1, slot_in, 1 - c)):
        pick = (lax.broadcasted_iota(jnp.int32, (slots, rows), 0) == ref[...]).astype(BF16)
        wave[h * rows:(h + 1) * rows] = dot_t(pick, arrived[owner].reshape(slots, width)).astype(BF16)

    order = (2 * far, 2 * far + 1, 2 * near, 2 * near + 1)
    ya = [flow(y_in.at[i], other_y) for i in range(BLOCKS)]
    rs_side = [flow(side_in.at[k], side) for k in range(len(UNITS))]
    rs_mid = [flow(mid_in.at[k], mid) for k in range(len(UNITS))]
    yb = [[flow(yb_in.at[q, part], other_y) for part in range(2)] for q in range(2)]

    def spot(h, kind, q, part):
        base = 0 if kind == "A" else width
        yy = 1 - y if kind == "P" else y
        return shared.at[2 * h + q, yy, :, pl.ds(base + part * hb, hb)]

    yg = [[flow(spot(near, "O", q, part), other_y) for part in range(2)] for q in range(2)]
    ga_y = [
        [[flow(spot(h, "A", q, part), other_y) for part in range(2)] for q in range(2)] for h in (near, far)
    ]
    out_h = z % 2
    ag_side = [flow(spot(out_h, *share), side) for share in SHARES]
    ag_side_in = [spot(1 - out_h, *share) for share in SHARES]
    ag_mid = [flow(spot(near, *share), mid) for share in SHARES]

    def own_unit(k, h, ysum_at):
        kind, q, yy, part = UNITS[k]
        if kind == "A":
            return y_sum[ysum_at + q, :, part * hb:(part + 1) * hb].astype(F32)
        return mine[2 * h + q, yy, :, width + part * hb:width + (part + 1) * hb].astype(F32)

    def project(i):
        b = order[i]
        x = dot(terms[b, 0], wave[...])
        v = dot(terms[b, 1], wave[...])

        def store(at, value):
            for yy in range(2):
                mine[b, yy, :, at:at + hb] = value[yy * half:(yy + 1) * half].astype(BF16)

        store(0, x[:, :hb] + v[:, hb:])
        store(hb, x[:, hb:] - v[:, :hb])
        ya[i].start(mine.at[b, 1 - y, :, pl.ds(0, width)])
        x = dot(terms[b, 2], wave[...])
        v = dot(terms[b, 3], wave[...])
        store(2 * hb, x[:, :hb] - v[:, hb:])
        store(3 * hb, x[:, hb:] + v[:, :hb])

    def head(kind, q):
        for k, unit in enumerate(UNITS):
            if unit[0] != kind or unit[1] != q:
                continue
            if kind == "A":
                rs_side[k].start(y_sum.at[q, :, pl.ds(unit[3] * hb, hb)])
            else:
                rs_side[k].start(mine.at[2 * far + q, unit[2], :, pl.ds(width + unit[3] * hb, hb)])

    def settle_y(i):
        ya[i].arrived()
        y_sum[i] = (mine[order[i], y, :, :width].astype(F32) + y_in[i].astype(F32)).astype(BF16)

    def inner_side(k):
        rs_side[k].arrived()
        side_in[k] = (side_in[k].astype(F32) + own_unit(k, far, 0)).astype(BF16)
        rs_mid[k].start(side_in.at[k])

    def inner_mid(k):
        rs_mid[k].arrived()
        mid_in[k] = (mid_in[k].astype(F32) + own_unit(k, near, 2)).astype(BF16)
        rs_side[k].start(mid_in.at[k])

    def couple(q, value):
        return exact_dot(coupling[q], value).astype(BF16)

    def share_at(kind, q, part):
        return SHARES.index((kind, q, part))

    def outer_side(k):
        kind, q, yy, part = UNITS[k]
        rs_side[k].arrived()
        value = side_in[k].astype(F32) + own_unit(k, near, 2)
        if kind == "A":
            spot(near, "A", q, part)[...] = couple(q, value)
            ag_side[share_at("A", q, part)].start(spot(near, "A", q, part))
            ga_y[0][q][part].start(spot(near, "A", q, part))
        else:
            side_in[k] = value.astype(BF16)

    def first_unit(q):
        return UNITS.index(("B", q, 0, 0))

    def outer_swap(q):
        for part in range(2):
            yb[q][part].start(side_in.at[first_unit(q) + 2 * (1 - y) + part])

    def outer_couple(q, part):
        yb[q][part].arrived()
        value = side_in[first_unit(q) + 2 * y + part].astype(F32) + yb_in[q, part].astype(F32)
        spot(near, "O", q, part)[...] = couple(q, value)
        yg[q][part].start(spot(near, "O", q, part))
        ag_side[share_at("O", q, part)].start(spot(near, "O", q, part))

    def outer_pass(q, part):
        yg[q][part].arrived()
        ag_side[share_at("P", q, part)].start(spot(near, "P", q, part))

    def inner_ag_side(k):
        kind, q, part = SHARES[k]
        ag_side[k].arrived()
        ag_mid[k].start(spot(near, *SHARES[k]))
        if kind == "A":
            ga_y[0][q][part].start(spot(near, *SHARES[k]))

    def inner_ag_mid(k):
        kind, q, part = SHARES[k]
        ag_mid[k].arrived()
        ag_side[k].start(spot(far, *SHARES[k]))
        if kind == "A":
            ga_y[1][q][part].start(spot(far, *SHARES[k]))

    def outer_ag(k):
        kind, q, part = SHARES[k]
        ag_side[k].arrived()
        if kind == "A":
            ga_y[1][q][part].start(spot(far, *SHARES[k]))

    done_left = set()

    def back(h, q, kind):
        which = (near, far)[h]
        if h == 0 and q == 0 and kind == "A":
            for copy in left_flows:
                copy.arrived()
        if kind == "A":
            for part in range(2):
                ga_y[h][q][part].arrived()
        b = 2 * which + q
        base, at = (0, 0) if kind == "A" else (width, 2)
        value = shared[b, :, :, base:base + width].reshape(plan.rows, width)
        x = dot(left[b, at], value)
        v = dot(left[b, at + 1], value)
        first = h == 0 and q == 0 and kind == "A"
        for part, term in ((0, x[:, :hb] - v[:, hb:]), (1, x[:, hb:] + v[:, :hb])):
            total[part] = term if first else total[part] + term

    def make_coupling():
        for q in range(2):
            atom = info[2 * near + q, pl.ds(pl.multiple_of(y * half, 8), half), 7:8]
            coupling[q] = coupling_matrix(plan, dmat_ref, spread, atom)

    events = schedule(
        project, head, settle_y, inner_side, inner_mid, outer_side, outer_swap, outer_couple, outer_pass,
        inner_ag_side, inner_ag_mid, outer_ag, back, make_coupling, prepare,
    )
    role_now, batch = None, []

    def flush():
        if not batch:
            return
        todo = list(batch)
        batch.clear()

        def run():
            for f, args in todo:
                f(*args)

        if role_now == "all":
            run()
        else:
            pl.when(outer if role_now == "outer" else inner)(run)

    for role, f, args in events:
        if role != role_now:
            flush()
            role_now = role
        batch.append((f, args))
    flush()

    out_flow = flow(out_in, other_core)
    for part in range(2):
        stage[part] = total[part, peer_rows].astype(BF16)
    out_flow.start(stage)
    for part in range(2):
        out_ref[part, :, pl.ds(pl.multiple_of(c * hb, hb), hb)] = total[part, own_rows].astype(BF16)
    out_flow.arrived()
    for part in range(2):
        out_ref[part, :, pl.ds(pl.multiple_of((1 - c) * hb, hb), hb)] = out_in[part]

    everyone = psi_flows + [slot_flow, g_flow, out_flow] + term_flows + left_flows + ya + rs_side + ag_side
    for pairs in ga_y:
        for pair in pairs:
            everyone += pair
    for copy in everyone:
        copy.sent()

    @pl.when(inner)
    def _():
        for copy in rs_mid + ag_mid:
            copy.sent()

    @pl.when(outer)
    def _():
        for pair in yb + yg:
            for copy in pair:
                copy.sent()


def schedule(
    project, head, settle_y, inner_side, inner_mid, outer_side, outer_swap, outer_couple, outer_pass,
    inner_ag_side, inner_ag_mid, outer_ag, back, make_coupling, prepare,
):
    events = []

    def at(time, role, f, *args):
        events.append((time, len(events), role, f, args))

    ready = COMPUTE * BLOCKS
    for i in range(BLOCKS):
        at(COMPUTE * i, "all", project, i)
        if i == 0:
            at(COMPUTE * i + 0.1, "outer", head, "B", 0)
    for i in range(BLOCKS):
        time = max(ready, COMPUTE + (i + 1) * 2 * UNIT + 2.0) + 0.01
        at(time, "all", settle_y, i)
        if i == 0:
            at(time + 0.001, "outer", head, "A", 0)
            at(time + 0.002, "outer", head, "B", 1)
        if i == 1:
            at(time + 0.001, "outer", head, "A", 1)
    settled = [max(ready, COMPUTE + (i + 1) * 2 * UNIT + 2.0) for i in range(BLOCKS)]

    def own_ready(k, i):
        return settled[i + UNITS[k][1]] if UNITS[k][0] == "A" else 0.0

    last_side, last_mid, last_out = 0.0, 0.0, 0.0
    out_time = []
    for k in range(len(UNITS)):
        last_side = max(COMPUTE + 2.0 + UNIT * (k + 1), last_side + UNIT, own_ready(k, 0) + 0.02)
        at(last_side, "inner", inner_side, k)
        last_mid = max(last_side + HOP, last_mid + UNIT, own_ready(k, 2) + 0.02)
        at(last_mid, "inner", inner_mid, k)
        last_out = max(last_mid + HOP, last_out + UNIT, own_ready(k, 2) + 0.02)
        at(last_out, "outer", outer_side, k)
        out_time.append(last_out)
    starts = {}
    for q in range(2):
        for part in range(2):
            k = UNITS.index(("A", q, 0, part))
            starts[("A", q, part)] = out_time[k] + 0.3
        swapped = out_time[UNITS.index(("B", q, 1, 1))] + 0.05
        at(swapped, "outer", outer_swap, q)
        for part in range(2):
            time = swapped + 2.0 + UNIT * (part + 1)
            at(time, "outer", outer_couple, q, part)
            starts[("O", q, part)] = time + 0.3
            at(time + HOP + 0.3, "outer", outer_pass, q, part)
            starts[("P", q, part)] = time + HOP + 0.4
    free = 0.0
    ready_at = {}
    for share in sorted(SHARES, key=lambda share: starts[share]):
        k = SHARES.index(share)
        free = max(free, starts[share]) + UNIT
        times = [free + 2.0, free + 2.0 + HOP, free + 2.0 + 2 * HOP]
        at(times[0], "inner", inner_ag_side, k)
        at(times[1], "inner", inner_ag_mid, k)
        at(times[2], "outer", outer_ag, k)
        ready_at[share] = (times[0], times[2])
    for h in range(2):
        for q in range(2):
            for kind in ("A", "B"):
                names = ("A",) if kind == "A" else ("O", "P")
                time = max(ready_at[(name, q, part)][h] for name in names for part in range(2))
                at(time + (HOP if kind == "A" else 0.0) + 0.01 * h, "all", back, h, q, kind)
    at(FILL[0], "outer", make_coupling)
    for b in range(EARLY, BLOCKS):
        at(FILL[b], "all", prepare, b)
    order = sorted(events, key=lambda event: event[:2])
    backs = [event for event in order if event[3] is back]
    first = next(event for event in backs if event[4] == (0, 0, "A"))
    if backs[0] is not first:
        place = order.index(backs[0])
        order.remove(first)
        order.insert(place, first)
    return [(role, f, args) for _, _, role, f, args in order]


def fused(plan, psi_k, send_index, recv_index, beta_k, beta_kq, displaced, mode, g_k, g_kq, dmat):
    rows, bands = psi_k.shape[1:]
    hb = bands // 2
    groups, cap = send_index.shape[1:]
    half = plan.half
    vmem = pl.BlockSpec(memory_space=pltpu.VMEM)
    units = len(UNITS)

    def buffer(*shape, dtype=BF16):
        return pltpu.VMEM(shape, dtype)

    return pl.pallas_call(
        functools.partial(fused_kernel, plan),
        in_specs=[vmem] * 8 + [pl.BlockSpec(memory_space=pl.ANY)] * 2,
        out_specs=vmem,
        out_shape=jax.ShapeDtypeStruct((2, rows, bands), BF16),
        scratch_shapes=[
            buffer(2 * rows, bands),
            buffer(BLOCKS, 4, plan.rows, 2 * rows),
            buffer(BLOCKS, 4, 2 * rows, plan.rows),
            buffer(BLOCKS, 2, half, 2 * bands),
            buffer(BLOCKS, half, bands),
            buffer(BLOCKS, half, bands),
            buffer(units, half, hb),
            buffer(units, half, hb),
            buffer(2, 2, half, hb),
            buffer(BLOCKS, 2, half, 2 * bands),
            buffer(2, 2 * rows, hb, dtype=F32),
            buffer(2, rows, hb),
            buffer(2, rows, hb),
            pltpu.VMEM(beta_k.shape, BF16),
            pltpu.VMEM(beta_kq.shape, BF16),
            buffer(groups // 2, 2, 2, cap, bands),
            buffer(2, groups, cap, bands),
            buffer(1, rows, dtype=jnp.int32),
            buffer(*g_k.shape, dtype=F32),
            buffer(8, displaced.shape[0], dtype=F32),
            buffer(BLOCKS, plan.rows, 8, dtype=F32),
            buffer(plan.per_atom * round_up(plan.per_atom, 8), dmat.shape[0], dtype=F32),
            buffer(2, half, half, dtype=F32),
            pltpu.SemaphoreType.DMA((COPIES,)),
            pltpu.SemaphoreType.DMA((COPIES,)),
            pltpu.SemaphoreType.DMA((2,)),
        ],
        compiler_params=params(collective_id=0, has_side_effects=True),
    )(
        psi_k, send_index[0], recv_index.reshape(1, -1), displaced.reshape(1, -1), mode, g_k, g_kq,
        jnp.transpose(dmat, (1, 2, 0)), beta_k, beta_kq,
    )


def pad_rows(layout, values, fill):
    k = values.shape[0]
    parts = values.reshape(k, layout.groups, layout.used)
    parts = jnp.pad(parts, ((0, 0), (0, 0), (0, layout.rows - layout.used)), constant_values=fill)
    parts = parts.reshape(k, layout.blocks, layout.block)
    parts = jnp.pad(parts, ((0, 0), (0, 0), (0, layout.padded - layout.block)), constant_values=fill)
    return parts.reshape(k, layout.blocks * layout.padded)


def block_coupling(layout, dmat, atoms):
    mine = lax.dynamic_slice_in_dim(atoms, lax.axis_index("ga") * layout.per_shard, layout.per_shard)
    blocks = jnp.take(dmat, mine, axis=0)
    eye = jnp.eye(layout.per_shard, dtype=F32)
    full = (blocks[:, :, None, :] * eye[:, None, :, None]).reshape(layout.used, layout.used)
    extra = layout.rows - layout.used
    return jnp.pad(full, ((0, extra), (0, extra)))


def on_device(psi_k, beta_k, beta_kq, g_k, g_kq, send_index, recv_index, dmat, displaced, mode):
    groups = lax.axis_size("ga")
    total = beta_k.shape[2]
    rows = beta_k.shape[1]
    per_atom = dmat.shape[1]
    beta_k, beta_kq = jnp.transpose(beta_k, (0, 2, 1)), jnp.transpose(beta_kq, (0, 2, 1))
    if groups == 4 * LINE:
        plan = Plan(displaced.shape[0], per_atom, total)
        return fused(plan, psi_k, send_index, recv_index, beta_k, beta_kq, displaced, mode, g_k, g_kq, dmat)

    layout = Layout(groups, displaced.shape[0], per_atom, total)

    packed = pack_rows(send_index.reshape(1, -1), psi_k)
    arrived = lax.all_to_all(packed, "ga", split_axis=0, concat_axis=0, tiled=True)

    rank = jnp.sum((displaced[None, :] < displaced[:, None]).astype(jnp.int32), axis=1)
    place = rank[None, :] == jnp.arange(displaced.shape[0], dtype=jnp.int32)[:, None]
    atoms = jnp.sum(jnp.where(place, displaced[None, :], 0), axis=1)
    moves = jnp.sum(jnp.where(place[None], mode[:, None, :], 0.0), axis=2)
    steps = jnp.tile(jnp.arange(per_atom, dtype=F32), displaced.shape[0])
    source = jnp.repeat(atoms.astype(F32) * per_atom, per_atom) + steps
    source = pad_rows(layout, source[None], -1.0)
    weights = pad_rows(layout, jnp.repeat(moves, per_atom, axis=1), 0.0)
    filler = jnp.zeros((8 - 1 - weights.shape[0], source.shape[1]), F32)
    info = jnp.concatenate([source, weights, filler], axis=0)
    coupling = block_coupling(layout, dmat, atoms)
    return separate_steps(
        layout, arrived, recv_index.reshape(1, -1), beta_k, beta_kq, info, g_k, g_kq, coupling
    )


def solution(mesh):
    in_specs = (
        P(None, "ga", None),
        P(None, "ga", None),
        P(None, "ga", None),
        P(None, "ga"),
        P(None, "ga"),
        P("ga", None, None),
        P("ga"),
        P(),
        P("pert"),
        P(None, "pert"),
    )
    out_specs = P("pert", "ga", None)
    return jax.shard_map(
        on_device, mesh=mesh, in_specs=in_specs, out_specs=out_specs, check_vma=False
    )
```
